16 devices in a mesh: data: 2 (over z), stage: 8 (over y, x, core).
Axes of the slice: x: 2, y: 2, z: 2, core: 2. Of those that a mesh axis runs over, the one named last changes fastest.
Arguments:
- X: bfloat16 [32, 256, 1024], P('data'), parts along dimension 0
- G: bfloat16 [32, 256, 1024], P('data'), parts along dimension 0
- W1: bfloat16 [8, 1024, 4096], P('stage')
- W2: bfloat16 [8, 4096, 1024], P('stage')
Outputs:
- output 1: bfloat16 [32, 256, 1024], P('data'), parts along dimension 0
- output 2: bfloat16 [32, 256, 1024], P('data'), parts along dimension 0
- output 3: float32 [16, 1024, 4096], P(('data', 'stage')), parts along dimension 0
- output 4: float32 [16, 4096, 1024], P(('data', 'stage')), parts along dimension 0
There are 2 independent parts. The reference program is written for one: setup_inputs(seed, part) draws one part's arguments, and reference() takes and returns one part's arrays. A program takes and returns all parts, laid end to end along the dimension named above; an argument that names none is the same for every part.
All inputs are finite; a program needn't handle non-finite values.
Results may differ from the reference program's by a relative error of at most 0.0134431.
Values are sent between devices in bfloat16 or wider.
A program may use at most 1 GiB of HBM per device.

```python
import jax
import jax.numpy as jnp
from jax import lax

D = 1024
F = 4096
LAYERS = 8
M = 16
B = 256


def setup_inputs(seed: int = 0, part: int = 0) -> dict:
    key = jax.random.PRNGKey(seed)
    ks, kpb = jax.random.split(key)
    kp = jax.random.fold_in(kpb, part)
    kx, kg = jax.random.split(kp)
    k1, k2 = jax.random.split(ks)
    X = jax.random.normal(kx, (M, B, D), jnp.float32).astype(jnp.bfloat16)
    G = jax.random.normal(kg, (M, B, D), jnp.float32).astype(jnp.bfloat16)
    W1 = (jax.random.normal(k1, (LAYERS, D, F), jnp.float32) * D ** -0.5).astype(jnp.bfloat16)
    W2 = (jax.random.normal(k2, (LAYERS, F, D), jnp.float32) * (F * LAYERS) ** -0.5).astype(jnp.bfloat16)
    return {'X': X, 'G': G, 'W1': W1, 'W2': W2}


def _fwd_layer(h, w1, w2):
    z = jnp.dot(h, w1, preferred_element_type=jnp.float32)
    u = jax.nn.gelu(z, approximate=True).astype(jnp.bfloat16)
    return (h.astype(jnp.float32) + jnp.dot(u, w2, preferred_element_type=jnp.float32)).astype(jnp.bfloat16)


def _bwd_layer(h, g, w1, w2):
    z = jnp.dot(h, w1, preferred_element_type=jnp.float32)
    u, gelu_vjp = jax.vjp(lambda t: jax.nn.gelu(t, approximate=True), z)
    du = jnp.dot(g, w2.T, preferred_element_type=jnp.float32)
    dz = gelu_vjp(du)[0].astype(jnp.bfloat16)
    dw2 = jnp.dot(u.astype(jnp.bfloat16).T, g, preferred_element_type=jnp.float32)
    dw1 = jnp.dot(h.T, dz, preferred_element_type=jnp.float32)
    dh = (g.astype(jnp.float32) + jnp.dot(dz, w1.T, preferred_element_type=jnp.float32)).astype(jnp.bfloat16)
    return dh, dw1, dw2


def reference(X, G, W1, W2):
    def one(carry, xg):
        a1, a2 = carry
        x, g = xg

        def fstep(h, w):
            return _fwd_layer(h, w[0], w[1]), h
        y, hs = lax.scan(fstep, x, (W1, W2))

        def bstep(gh, inp):
            w1, w2, h, c1, c2 = inp
            dh, dw1, dw2 = _bwd_layer(h, gh, w1, w2)
            return dh, (c1 + dw1, c2 + dw2)
        dx, (a1, a2) = lax.scan(bstep, g, (W1, W2, hs, a1, a2), reverse=True)
        return (a1, a2), (y, dx)

    init = (jnp.zeros(W1.shape, jnp.float32), jnp.zeros(W2.shape, jnp.float32))
    (dW1, dW2), (Y, dX) = lax.scan(one, init, (X, G))
    return Y, dX, dW1, dW2
```

```python
import functools

import jax
import jax.numpy as jnp
from jax import lax
from jax.experimental import pallas as pl
from jax.experimental.pallas import tpu as pltpu
from jax.sharding import PartitionSpec as P

BF = jnp.bfloat16
F32 = jnp.float32
C0 = 0.7978845608028654
C1 = 0.044715
NT = (((1,), (1,)), ((), ()))
FT = 512
OT = 512
WARM = (16, 16, 16, 16, 10, 8, 3, 1)
LAG_Y = (0, 3, 0, 2, 0, 1, 0, 0)
LAG_X = (0, 0, 4, 0, 4, 0, 8, 0)


def _gelu(z):
    a = (C0 * C1) * (z * z)
    s = 0.5 * jnp.tanh(z * (a + C0)) + 0.5
    u = z * s
    return u, s + (u - u * s) * (6.0 * a + 2.0 * C0)


def _pick(s, table):
    out = jnp.int32(table[-1])
    for i, v in enumerate(table[:-1]):
        out = jnp.where(s == i, jnp.int32(v), out)
    return out


def _pipe(n, n_st, x, gin, w1h, w2h, y, dx, hs, gs, us, dzs, gps,
          w1, w2, h_all, g_all, u, gp, dz, of, ob,
          w_sem, h_recv, g_recv, y_recv, x_recv, hs_sem, gs_sem,
          u_sem, gp_sem, pf_sem, dz_sem, f_send, b_send,
          y_loc, y_send, x_loc, x_send, yr_send, xr_send):
    s = lax.axis_index('stage')
    first = s == 0
    last = s == n_st - 1
    w = _pick(s, WARM)
    lag_y = _pick(s, LAG_Y)
    lag_x = _pick(s, LAG_X)
    f_dim = w1.shape[1]
    d_dim = w1.shape[0]

    def local(src, dst, sem):
        return pltpu.make_async_copy(src, dst, sem)

    def remote(src, dst, ssem, rsem, dev):
        return pltpu.make_async_remote_copy(
            src_ref=src, dst_ref=dst, send_sem=ssem, recv_sem=rsem,
            device_id={'stage': dev}, device_id_type=pl.DeviceIdType.MESH)

    @pl.when(first)
    def _():
        local(x.at[0], h_all.at[0], h_recv.at[0]).start()
    local(w1h, w1, w_sem.at[0]).start()
    local(w2h, w2, w_sem.at[1]).start()

    @pl.when(first)
    def _():
        def go(m, c):
            local(x.at[m], h_all.at[m], h_recv.at[m]).start()
            return c
        lax.fori_loop(1, n, go, 0)

    @pl.when(last)
    def _():
        def go(m, c):
            local(gin.at[m], g_all.at[m], g_recv.at[m]).start()
            return c
        lax.fori_loop(0, n, go, 0)
    local(w1h, w1, w_sem.at[0]).wait()
    local(w2h, w2, w_sem.at[1]).wait()

    relay_y = (s == 1) | (s == 3) | (s == 5)
    relay_x = (s == 2) | (s == 4) | (s == 6)

    def pass_y(m):
        local(y.at[m], y.at[m], y_recv.at[m]).wait()

        @pl.when(relay_y)
        def _():
            remote(y.at[m], y.at[m], yr_send.at[0, m], y_recv.at[m], s - 1).start()

        @pl.when(s == 5)
        def _():
            remote(y.at[m], y.at[m], yr_send.at[1, m], y_recv.at[m], 1).start()

    def pass_x(m):
        local(dx.at[m], dx.at[m], x_recv.at[m]).wait()

        @pl.when(relay_x)
        def _():
            remote(dx.at[m], dx.at[m], xr_send.at[0, m], x_recv.at[m], s + 1).start()

        @pl.when(s == 2)
        def _():
            remote(dx.at[m], dx.at[m], xr_send.at[1, m], x_recv.at[m], 6).start()

    def wait_f_send(sl):
        @pl.when(last)
        def _():
            local(of.at[sl], y.at[0], y_loc.at[sl]).wait()
            for k, dev in enumerate((6, 5, 3)):
                remote(of.at[sl], y.at[0], y_send.at[k, sl], y_recv.at[0], dev).wait_send()

        @pl.when(jnp.logical_not(last))
        def _():
            remote(of.at[sl], h_all.at[0], f_send.at[sl], h_recv.at[0], s + 1).wait_send()

    def wait_b_send(sl):
        @pl.when(first)
        def _():
            local(ob.at[sl], dx.at[0], x_loc.at[sl]).wait()
            for k, dev in enumerate((1, 2, 4)):
                remote(ob.at[sl], dx.at[0], x_send.at[k, sl], x_recv.at[0], dev).wait_send()

        @pl.when(jnp.logical_not(first))
        def _():
            remote(ob.at[sl], g_all.at[0], b_send.at[sl], g_recv.at[0], s - 1).wait_send()

    def wait_f_store(sl):
        local(u.at[sl], us.at[0], u_sem.at[sl]).wait()
        local(gp.at[sl], gps.at[0], gp_sem.at[sl]).wait()

    def forward(m):
        sl = m % 2
        local(h_all.at[m], h_all.at[m], h_recv.at[m]).wait()
        local(h_all.at[m], hs.at[m], hs_sem).start()

        @pl.when(m >= 2)
        def _():
            wait_f_send(sl)
        h = h_all.at[m]
        for j in range(f_dim // FT):
            c = pl.ds(j * FT, FT)
            z = jnp.dot(h[...], w1[:, c], preferred_element_type=F32)
            uu, gg = _gelu(z)
            u[sl, :, c] = uu.astype(BF)
            gp[sl, :, c] = gg
        for j in range(d_dim // OT):
            c = pl.ds(j * OT, OT)
            r = jnp.dot(u[sl], w2[:, c], preferred_element_type=F32)
            of[sl, :, c] = (h[:, c].astype(F32) + r).astype(BF)

        @pl.when(last)
        def _():
            for k, dev in enumerate((6, 5, 3)):
                remote(of.at[sl], y.at[m], y_send.at[k, sl], y_recv.at[m], dev).start()
            local(of.at[sl], y.at[m], y_loc.at[sl]).start()

        @pl.when(jnp.logical_not(last))
        def _():
            remote(of.at[sl], h_all.at[m], f_send.at[sl], h_recv.at[m], s + 1).start()
        local(u.at[sl], us.at[m], u_sem.at[sl]).start()
        local(gp.at[sl], gps.at[m], gp_sem.at[sl]).start()

    def backward(m):
        sl = m % 2
        gi = jnp.where(w == 1, sl, 2)
        local(g_all.at[m], g_all.at[m], g_recv.at[m]).wait()
        local(g_all.at[m], gs.at[m], gs_sem).start()

        @pl.when(w > 1)
        def _():
            local(gps.at[m], gp.at[2], pf_sem).wait()

        @pl.when(m >= 2)
        def _():
            wait_b_send(sl)
            local(dz.at[sl], dzs.at[0], dz_sem.at[sl]).wait()
        g = g_all.at[m]
        for j in range(f_dim // FT):
            c = pl.ds(j * FT, FT)
            du = lax.dot_general(g[...], w2[c, :], NT, preferred_element_type=F32)
            dz[sl, :, c] = (gp[gi, :, c] * du).astype(BF)
        for j in range(d_dim // OT):
            c = pl.ds(j * OT, OT)
            r = lax.dot_general(dz[sl], w1[c, :], NT, preferred_element_type=F32)
            ob[sl, :, c] = (g[:, c].astype(F32) + r).astype(BF)

        @pl.when(first)
        def _():
            for k, dev in enumerate((1, 2, 4)):
                remote(ob.at[sl], dx.at[m], x_send.at[k, sl], x_recv.at[m], dev).start()
            local(ob.at[sl], dx.at[m], x_loc.at[sl]).start()

        @pl.when(jnp.logical_not(first))
        def _():
            remote(ob.at[sl], g_all.at[m], b_send.at[sl], g_recv.at[m], s - 1).start()
        local(dz.at[sl], dzs.at[m], dz_sem.at[sl]).start()

    ticks = n + jnp.maximum(w, 2)

    def tick(t, c):
        @pl.when((t >= 2) & (t < n + 2))
        def _():
            wait_f_store(t % 2)

        @pl.when((t >= w) & (t - w < n))
        def _():
            backward(t - w)

        @pl.when((w > 1) & (t - w + 1 >= 0) & (t - w + 1 < n))
        def _():
            local(gps.at[t - w + 1], gp.at[2], pf_sem).start()

        @pl.when(t < n)
        def _():
            forward(t)

        my = t - w - lag_y

        @pl.when(relay_y & (my >= 0) & (my < n))
        def _():
            pass_y(my)
        mx = t - w - lag_x

        @pl.when(relay_x & (mx >= 0) & (mx < n))
        def _():
            pass_x(mx)
        return c
    lax.fori_loop(0, ticks, tick, 0)

    y0 = jnp.where(relay_y, jnp.clip(ticks - w - lag_y, 0, n), jnp.where(last, n, 0))
    x0 = jnp.where(relay_x, jnp.clip(ticks - w - lag_x, 0, n), jnp.where(first, n, 0))

    def rest_y(m, c):
        pass_y(m)
        return c

    def rest_x(m, c):
        pass_x(m)
        return c
    lax.fori_loop(y0, n, rest_y, 0)
    lax.fori_loop(x0, n, rest_x, 0)
    for m in (n - 2, n - 1):
        wait_f_send(m % 2)
        wait_b_send(m % 2)
        local(dz.at[m % 2], dzs.at[0], dz_sem.at[m % 2]).wait()
    local(h_all, hs, hs_sem).wait()
    local(g_all, gs, gs_sem).wait()

    def done(m, c):
        @pl.when(relay_y)
        def _():
            remote(y.at[m], y.at[m], yr_send.at[0, m], y_recv.at[m], s - 1).wait_send()

        @pl.when(s == 5)
        def _():
            remote(y.at[m], y.at[m], yr_send.at[1, m], y_recv.at[m], 1).wait_send()

        @pl.when(relay_x)
        def _():
            remote(dx.at[m], dx.at[m], xr_send.at[0, m], x_recv.at[m], s + 1).wait_send()

        @pl.when(s == 2)
        def _():
            remote(dx.at[m], dx.at[m], xr_send.at[1, m], x_recv.at[m], 6).wait_send()
        return c
    lax.fori_loop(0, n, done, 0)


def _run_pipe(n_st, x, g, w1, w2):
    n, b, d = x.shape
    f = w1.shape[1]
    act = jax.ShapeDtypeStruct((n, b, d), BF)
    wide = jax.ShapeDtypeStruct((n, b, f), BF)
    anyspec = pl.BlockSpec(memory_space=pl.ANY)
    dma = pltpu.SemaphoreType.DMA
    return pl.pallas_call(
        functools.partial(_pipe, n, n_st),
        out_shape=(act, act, act, act, wide, wide, jax.ShapeDtypeStruct((n, b, f), F32)),
        in_specs=[anyspec] * 4,
        out_specs=(anyspec,) * 7,
        scratch_shapes=[
            pltpu.VMEM((d, f), BF), pltpu.VMEM((f, d), BF),
            pltpu.VMEM((n, b, d), BF), pltpu.VMEM((n, b, d), BF),
            pltpu.VMEM((2, b, f), BF), pltpu.VMEM((3, b, f), F32), pltpu.VMEM((2, b, f), BF),
            pltpu.VMEM((2, b, d), BF), pltpu.VMEM((2, b, d), BF),
            dma((2,)), dma((n,)), dma((n,)), dma((n,)), dma((n,)), dma, dma,
            dma((2,)), dma((2,)), dma, dma((2,)), dma((2,)), dma((2,)),
            dma((2,)), dma((3, 2)), dma((2,)), dma((3, 2)), dma((2, n)), dma((2, n)),
        ],
        compiler_params=pltpu.CompilerParams(has_side_effects=True, vmem_limit_bytes=63 * 1024 * 1024),
    )(x, g, w1, w2)


def solution(mesh):
    n_st = mesh.shape['stage']

    def body(x, g, w1, w2):
        n, b, d = x.shape
        f = w1.shape[2]
        y, dx, hs, gs, us, dzs, _ = _run_pipe(n_st, x, g, w1[0], w2[0])
        tn = (((0,), (0,)), ((), ()))
        hs, gs = hs.reshape(n * b, d), gs.reshape(n * b, d)
        us, dzs = us.reshape(n * b, f), dzs.reshape(n * b, f)
        dw1 = lax.dot_general(hs, dzs, tn, preferred_element_type=F32)
        dw2 = lax.dot_general(us, gs, tn, preferred_element_type=F32)
        return y, dx, dw1[None], dw2[None]

    return jax.shard_map(body, mesh=mesh,
                         in_specs=(P('data'), P('data'), P('stage'), P('stage')),
                         out_specs=(P('data'), P('data'), P(('data', 'stage')), P(('data', 'stage'))),
                         check_vma=False)
```

```python
import functools

import jax
import jax.numpy as jnp
from jax import lax
from jax.experimental import pallas as pl
from jax.experimental.pallas import tpu as pltpu
from jax.sharding import PartitionSpec as P

BF = jnp.bfloat16
F32 = jnp.float32
C0 = 0.7978845608028654
C1 = 0.044715
NT = (((1,), (1,)), ((), ()))
TN = (((0,), (0,)), ((), ()))
FT = 512
OT = 512
WARM = (16, 16, 16, 16, 11, 9, 3, 1)
KB = 8
PAR_Y = (0, 0, 0, 1, 0, 0, 0, 0)
OFF_P = (99, 17, 99, 16, 99, 14, 99, 99)
OFF_S = (99, 17, 99, 22, 99, 21, 99, 99)
LAG_X = (0, 0, 5, 0, 7, 0, 12, 0)
NF = 4
T_W = (25, 25, 28, 32, 27, 25, 19, 18)
YC = 12
LATE_Y = {20: 12, 21: 14, 23: 13, 24: 15}


def _gelu(z):
    a = (C0 * C1) * (z * z)
    s = 0.5 * jnp.tanh(z * (a + C0)) + 0.5
    u = z * s
    return u, s + (u - u * s) * (6.0 * a + 2.0 * C0)


def _pick(s, table):
    out = jnp.int32(table[-1])
    for i, v in enumerate(table[:-1]):
        out = jnp.where(s == i, jnp.int32(v), out)
    return out


def _pipe(n, n_st, x, gin, w1h, w2h, y, dx, hs, gs, us, dzs, gps, p1, p2,
          w1, w2, h_all, g_all, u, gp, dz, of, ob,
          w_sem, h_recv, g_recv, y_recv, x_recv, hs_sem, gs_sem,
          u_sem, gp_sem, pf_sem, dz_sem, f_send, b_send,
          y_loc, y_send, x_loc, x_send, yr_send, xr_send, wu_sem, wd_sem, wo_sem):
    s = lax.axis_index('stage')
    first = s == 0
    last = s == n_st - 1
    w = _pick(s, WARM)
    par_y = _pick(s, PAR_Y)
    off_p = _pick(s, OFF_P)
    off_s = _pick(s, OFF_S)
    lag_x = _pick(s, LAG_X)
    f_dim = w1.shape[1]
    d_dim = w1.shape[0]

    def local(src, dst, sem):
        return pltpu.make_async_copy(src, dst, sem)

    def remote(src, dst, ssem, rsem, dev):
        return pltpu.make_async_remote_copy(
            src_ref=src, dst_ref=dst, send_sem=ssem, recv_sem=rsem,
            device_id={'stage': dev}, device_id_type=pl.DeviceIdType.MESH)

    @pl.when(first)
    def _():
        local(x.at[0], h_all.at[0], h_recv.at[0]).start()
    local(w1h, w1, w_sem.at[0]).start()
    local(w2h, w2, w_sem.at[1]).start()

    @pl.when(last)
    def _():
        def go(m, c):
            local(gin.at[m], g_all.at[m], g_recv.at[m]).start()
            return c
        lax.fori_loop(0, n, go, 0)
    local(w1h, w1, w_sem.at[0]).wait()
    local(w2h, w2, w_sem.at[1]).wait()

    @pl.when(first)
    def _():
        def go(m, c):
            local(x.at[m], h_all.at[m], h_recv.at[m]).start()
            return c
        lax.fori_loop(1, n, go, 0)

    relay_y = (s == 1) | (s == 3) | (s == 5)
    relay_x = (s == 2) | (s == 4) | (s == 6)

    def second_y(m):
        return (s == 1) | ((s == 5) & (m % 2 == 0)) | ((s == 3) & (m % 2 == 1))

    def next_y(m):
        return jnp.where(s == 1, 3 + 2 * (m % 2), 1)

    def pass_y(m):
        local(y.at[m], y.at[m], y_recv.at[m]).wait()

        @pl.when(relay_y)
        def _():
            remote(y.at[m], y.at[m], yr_send.at[0, m], y_recv.at[m], s - 1).start()

        @pl.when(second_y(m))
        def _():
            remote(y.at[m], y.at[m], yr_send.at[1, m], y_recv.at[m], next_y(m)).start()

    def pass_x(m):
        local(dx.at[m], dx.at[m], x_recv.at[m]).wait()

        @pl.when(relay_x)
        def _():
            remote(dx.at[m], dx.at[m], xr_send.at[0, m], x_recv.at[m], s + 1).start()

        @pl.when(s == 2)
        def _():
            remote(dx.at[m], dx.at[m], xr_send.at[1, m], x_recv.at[m], 6).start()

    def wait_f_send(sl):
        remote(of.at[sl], h_all.at[0], f_send.at[sl], h_recv.at[0], s + 1).wait_send()

    def wait_b_send(sl):
        @pl.when(first)
        def _():
            local(ob.at[sl], dx.at[0], x_loc.at[sl]).wait()
            for k, dev in enumerate((1, 2, 4)):
                remote(ob.at[sl], dx.at[0], x_send.at[k, sl], x_recv.at[0], dev).wait_send()

        @pl.when(jnp.logical_not(first))
        def _():
            remote(ob.at[sl], g_all.at[0], b_send.at[sl], g_recv.at[0], s - 1).wait_send()

    def wait_f_store(sl):
        local(u.at[sl], us.at[0], u_sem.at[sl]).wait()
        local(gp.at[sl], gps.at[0], gp_sem.at[sl]).wait()

    def forward(m):
        sl = m % NF
        su = m % 2
        local(h_all.at[m], h_all.at[m], h_recv.at[m]).wait()
        local(h_all.at[m], hs.at[m], hs_sem).start()

        @pl.when(jnp.logical_not(last) & (m >= NF))
        def _():
            wait_f_send(sl)
        h = h_all.at[m]
        with jax.named_scope('F'):
            for j in range(f_dim // FT):
                c = pl.ds(j * FT, FT)
                z = jnp.dot(h[...], w1[:, c], preferred_element_type=F32)
                uu, gg = _gelu(z)
                u[su, :, c] = uu.astype(BF)
                gp[su, :, c] = gg
            for j in range(d_dim // OT):
                c = pl.ds(j * OT, OT)
                r = jnp.dot(u[su], w2[:, c], preferred_element_type=F32)
                of[sl, :, c] = (h[:, c].astype(F32) + r).astype(BF)

        @pl.when(last)
        def _():
            local(of.at[sl], y.at[m], y_loc.at[sl]).start()

        @pl.when(jnp.logical_not(last))
        def _():
            remote(of.at[sl], h_all.at[m], f_send.at[sl], h_recv.at[m], s + 1).start()
        local(u.at[su], us.at[m], u_sem.at[su]).start()
        local(gp.at[su], gps.at[m], gp_sem.at[su]).start()

    def backward(m):
        sl = m % 2
        gi = jnp.where(w == 1, sl, 2)
        local(g_all.at[m], g_all.at[m], g_recv.at[m]).wait()
        local(g_all.at[m], gs.at[m], gs_sem).start()

        @pl.when(w > 1)
        def _():
            local(gps.at[m], gp.at[2], pf_sem).wait()

        @pl.when(m >= 2)
        def _():
            wait_b_send(sl)

        @pl.when(m >= 1)
        def _():
            local(dz, dzs.at[0], dz_sem).wait()
        g = g_all.at[m]
        with jax.named_scope('B'):
            for j in range(f_dim // FT):
                c = pl.ds(j * FT, FT)
                du = lax.dot_general(g[...], w2[c, :], NT, preferred_element_type=F32)
                dz[:, c] = (gp[gi, :, c] * du).astype(BF)
            local(dz, dzs.at[m], dz_sem).start()
            for j in range(d_dim // OT):
                c = pl.ds(j * OT, OT)
                r = lax.dot_general(dz[...], w1[c, :], NT, preferred_element_type=F32)
                ob[sl, :, c] = (g[:, c].astype(F32) + r).astype(BF)

        @pl.when(first)
        def _():
            for k, dev in enumerate((1, 2, 4)):
                remote(ob.at[sl], dx.at[m], x_send.at[k, sl], x_recv.at[m], dev).start()
            local(ob.at[sl], dx.at[m], x_loc.at[sl]).start()

        @pl.when(jnp.logical_not(first))
        def _():
            remote(ob.at[sl], g_all.at[m], b_send.at[sl], g_recv.at[m], s - 1).start()

    n_grp = f_dim // FT

    def w_load(i):
        c = pl.ds(pl.multiple_of(i * FT, FT), FT)
        sl = i % 2
        for k in range(KB):
            to = pl.ds(k * FT, FT)
            local(us.at[k, :, c], u.at[2 * sl, :, to], wu_sem.at[sl]).start()
            local(dzs.at[k, :, c], u.at[2 * sl + 1, :, to], wd_sem.at[sl]).start()

    def w_group(i):
        sl = i % 2

        @pl.when(i + 1 < n_grp)
        def _():
            w_load(i + 1)
        local(us.at[0], u.at[2 * sl], wu_sem.at[sl]).wait()
        local(dzs.at[0], u.at[2 * sl + 1], wd_sem.at[sl]).wait()

        @pl.when(i >= 2)
        def _():
            local(gp.at[sl], gps.at[0], wo_sem.at[sl]).wait()
        kt = KB * h_all.shape[1]
        b = h_all.shape[1]
        with jax.named_scope('W'):
            lhs = jnp.concatenate([u[2 * sl, :, k * FT:(k + 1) * FT] for k in range(KB)], axis=0)
            r = lax.dot_general(lhs, g_all[0:KB].reshape(kt, d_dim), TN, preferred_element_type=F32)
            for q in range(FT // b):
                gp[sl, :, d_dim * q:d_dim * (q + 1)] = r[b * q:b * (q + 1)]
            rhs = jnp.concatenate([u[2 * sl + 1, :, k * FT:(k + 1) * FT] for k in range(KB)], axis=0)
            r = lax.dot_general(h_all[0:KB].reshape(kt, d_dim), rhs, TN, preferred_element_type=F32)
            for q in range(d_dim // b):
                gp[sl, :, 2 * d_dim + FT * q:2 * d_dim + FT * (q + 1)] = r[b * q:b * (q + 1)]
        for q in range(FT // b):
            local(gp.at[sl, :, pl.ds(d_dim * q, d_dim)],
                  p2.at[pl.ds(pl.multiple_of(i * FT + b * q, b), b), :], wo_sem.at[sl]).start()
        for q in range(d_dim // b):
            local(gp.at[sl, :, pl.ds(2 * d_dim + FT * q, FT)],
                  p1.at[pl.ds(b * q, b), pl.ds(pl.multiple_of(i * FT, FT), FT)], wo_sem.at[sl]).start()

    t0 = _pick(s, T_W)
    ticks = jnp.maximum(jnp.maximum(n + w, t0 + n_grp), n + 2)

    def send_y(m):
        remote(y.at[m], y.at[m], y_send.at[0, m], y_recv.at[m], 6).start()
        remote(y.at[m], y.at[m], y_send.at[1, m], y_recv.at[m], 5 - 2 * (m % 2)).start()

    def tick(t, c):
        @pl.when((t >= 2) & (t < n + 2))
        def _():
            wait_f_store(t % 2)

        @pl.when(last & (t >= 2) & (t < n + 2))
        def _():
            local(of.at[(t - 2) % NF], y.at[0], y_loc.at[(t - 2) % NF]).wait()

            @pl.when(t - 2 < YC)
            def _():
                send_y(t - 2)
        for at, m in LATE_Y.items():
            @pl.when(last & (t == at))
            def _(m=m):
                send_y(m)

        @pl.when((t >= w) & (t - w < n))
        def _():
            backward(t - w)

        @pl.when((w > 1) & (t - w + 1 >= 0) & (t - w + 1 < n))
        def _():
            local(gps.at[t - w + 1], gp.at[2], pf_sem).start()

        @pl.when(t < n)
        def _():
            forward(t)

        @pl.when((t >= t0) & (t < t0 + n_grp))
        def _():
            w_group(t - t0)

        @pl.when(t == t0 - 1)
        def _():
            w_load(0)

        mp = t - off_p

        @pl.when((mp >= 0) & (mp < YC) & (mp % 2 == par_y))
        def _():
            pass_y(mp)
        ml = t - (n + w + 2) + YC

        @pl.when(relay_y & (ml >= YC) & (ml < n) & (ml % 2 == par_y))
        def _():
            pass_y(ml)
        ms = t - off_s

        @pl.when((ms >= 0) & (ms < YC) & (ms % 2 != par_y))
        def _():
            pass_y(ms)
        mx = t - w - lag_x

        @pl.when(relay_x & (mx >= 0) & (mx < n))
        def _():
            pass_x(mx)
        return c
    lax.fori_loop(0, ticks, tick, 0)

    x0 = jnp.where(relay_x, jnp.clip(ticks - w - lag_x, 0, n), jnp.where(first, n, 0))

    def left_p(m):
        at = jnp.where(m < YC, m + off_p, jnp.where(relay_y, n + w + 2 + m - YC, 999))
        return (m % 2 == par_y) & (at >= ticks)

    def left_s(m):
        at = jnp.where(m < YC, m + off_s, 999)
        return (m % 2 != par_y) & (at >= ticks)

    def rest_p(m, c):
        @pl.when(left_p(m) | ((s == 1) & left_s(m)))
        def _():
            pass_y(m)
        return c

    def rest_s(m, c):
        @pl.when(left_s(m) & (s != 1))
        def _():
            pass_y(m)
        return c

    def rest_x(m, c):
        pass_x(m)
        return c
    early = jnp.where(relay_y, 0, n)
    late = jnp.where(relay_y | last, n, 0)
    lax.fori_loop(early, n, rest_p, 0)
    lax.fori_loop(early, n, rest_s, 0)
    lax.fori_loop(x0, n, rest_x, 0)
    lax.fori_loop(late, n, rest_p, 0)
    lax.fori_loop(late, n, rest_s, 0)

    @pl.when(jnp.logical_not(last))
    def _():
        for m in range(n - NF, n):
            wait_f_send(m % NF)
    for m in (n - 2, n - 1):
        wait_b_send(m % 2)
        local(gp.at[m % 2], gps.at[0], wo_sem.at[m % 2]).wait()
    local(dz, dzs.at[0], dz_sem).wait()
    local(h_all, hs, hs_sem).wait()
    local(g_all, gs, gs_sem).wait()

    def done(m, c):
        @pl.when(last)
        def _():
            for k in range(2):
                remote(y.at[m], y.at[m], y_send.at[k, m], y_recv.at[m], 6).wait_send()

        @pl.when(relay_y)
        def _():
            remote(y.at[m], y.at[m], yr_send.at[0, m], y_recv.at[m], s - 1).wait_send()

        @pl.when(second_y(m))
        def _():
            remote(y.at[m], y.at[m], yr_send.at[1, m], y_recv.at[m], next_y(m)).wait_send()

        @pl.when(relay_x)
        def _():
            remote(dx.at[m], dx.at[m], xr_send.at[0, m], x_recv.at[m], s + 1).wait_send()

        @pl.when(s == 2)
        def _():
            remote(dx.at[m], dx.at[m], xr_send.at[1, m], x_recv.at[m], 6).wait_send()
        return c
    lax.fori_loop(0, n, done, 0)


def _run_pipe(n_st, x, g, w1, w2):
    n, b, d = x.shape
    f = w1.shape[1]
    act = jax.ShapeDtypeStruct((n, b, d), BF)
    wide = jax.ShapeDtypeStruct((n, b, f), BF)
    anyspec = pl.BlockSpec(memory_space=pl.ANY)
    dma = pltpu.SemaphoreType.DMA
    return pl.pallas_call(
        functools.partial(_pipe, n, n_st),
        out_shape=(act, act, act, act, wide, wide, jax.ShapeDtypeStruct((n, b, f), F32),
                   jax.ShapeDtypeStruct((d, f), F32), jax.ShapeDtypeStruct((f, d), F32)),
        in_specs=[anyspec] * 4,
        out_specs=(anyspec,) * 9,
        scratch_shapes=[
            pltpu.VMEM((d, f), BF), pltpu.VMEM((f, d), BF),
            pltpu.VMEM((n, b, d), BF), pltpu.VMEM((n, b, d), BF),
            pltpu.VMEM((4, b, f), BF), pltpu.VMEM((3, b, f), F32), pltpu.VMEM((b, f), BF),
            pltpu.VMEM((NF, b, d), BF), pltpu.VMEM((2, b, d), BF),
            dma((2,)), dma((n,)), dma((n,)), dma((n,)), dma((n,)), dma, dma,
            dma((2,)), dma((2,)), dma, dma, dma((NF,)), dma((2,)),
            dma((NF,)), dma((2, n)), dma((2,)), dma((3, 2)), dma((2, n)), dma((2, n)),
            dma((2,)), dma((2,)), dma((2,)),
        ],
        compiler_params=pltpu.CompilerParams(has_side_effects=True, vmem_limit_bytes=67043328),
    )(x, g, w1, w2)


def _finish(u, dz, h, g, p1, p2, y, dx, o1, o2, yo, dxo):
    o2[...] = p2[...] + lax.dot_general(u[...], g[...], TN, preferred_element_type=F32)
    o1[...] = p1[...] + lax.dot_general(h[...], dz[...], TN, preferred_element_type=F32)
    yo[...] = y[...]
    dxo[...] = dx[...]


def _run_finish(us, dzs, hs, gs, p1, p2, y, dx):
    n, b, d = y.shape
    f = us.shape[1]
    k = (n - KB) * b
    steps = f // FT
    m = n // steps
    one = pl.Buffered(1)
    act = pl.BlockSpec((m, b, d), lambda j: (j, 0, 0))
    col = pl.BlockSpec((d, FT), lambda j: (0, j))
    row = pl.BlockSpec((FT, d), lambda j: (j, 0))
    tok = pl.BlockSpec((k, FT), lambda j: (1, j))
    all_d = pl.BlockSpec((k, d), lambda j: (1, 0), pipeline_mode=one)
    return pl.pallas_call(
        _finish,
        grid=(steps,),
        out_shape=(jax.ShapeDtypeStruct((d, f), F32), jax.ShapeDtypeStruct((f, d), F32),
                   jax.ShapeDtypeStruct((n, b, d), BF), jax.ShapeDtypeStruct((n, b, d), BF)),
        in_specs=[tok, tok, all_d, all_d, col, row, act, act],
        out_specs=[col, row, act, act],
        compiler_params=pltpu.CompilerParams(vmem_limit_bytes=63 * 1024 * 1024),
    )(us, dzs, hs, gs, p1, p2, y, dx)


def solution(mesh):
    n_st = mesh.shape['stage']

    def body(x, g, w1, w2):
        n, b, d = x.shape
        f = w1.shape[2]
        y, dx, hs, gs, us, dzs, _, p1, p2 = _run_pipe(n_st, x, g, w1[0], w2[0])
        dw1, dw2, y, dx = _run_finish(us.reshape(n * b, f), dzs.reshape(n * b, f), hs.reshape(n * b, d),
                                      gs.reshape(n * b, d), p1, p2, y, dx)
        return y, dx, dw1[None], dw2[None]

    return jax.shard_map(body, mesh=mesh,
                         in_specs=(P('data'), P('data'), P('stage'), P('stage')),
                         out_specs=(P('data'), P('data'), P(('data', 'stage')), P(('data', 'stage'))),
                         check_vma=False)
```

```python
import functools

import jax
import jax.numpy as jnp
from jax import lax
from jax.experimental import pallas as pl
from jax.experimental.pallas import tpu as pltpu
from jax.sharding import PartitionSpec as P

BF = jnp.bfloat16
F32 = jnp.float32
C0 = 0.7978845608028654
C1 = 0.044715
NT = (((1,), (1,)), ((), ()))
TN = (((0,), (0,)), ((), ()))
FT = 512
OT = 512
WARM = (16, 16, 16, 16, 11, 9, 3, 1)
KB = 8
PAR_Y = (0, 0, 0, 1, 0, 0, 0, 0)
OFF_P = (99, 17, 99, 16, 99, 14, 99, 99)
OFF_S = (99, 17, 99, 22, 99, 21, 99, 99)
LAG_X = (0, 0, 5, 0, 7, 0, 12, 0)
NF = 4
T_W = (25, 25, 28, 32, 27, 25, 19, 18)
YC = 12
LATE_Y = {20: 12, 21: 14, 23: 13, 24: 15}


def _gelu(z):
    a = (C0 * C1) * (z * z)
    s = 0.5 * jnp.tanh(z * (a + C0)) + 0.5
    u = z * s
    return u, s + (u - u * s) * (6.0 * a + 2.0 * C0)


def _pick(s, table):
    out = jnp.int32(table[-1])
    for i, v in enumerate(table[:-1]):
        out = jnp.where(s == i, jnp.int32(v), out)
    return out


def _pipe(n, n_st, x, gin, w1h, w2h, y, dx, hs, gs, us, dzs, gps, p1, p2,
          w1, w2, h_all, g_all, u, gp, dz, of, ob,
          w_sem, h_recv, g_recv, y_recv, x_recv, hs_sem, gs_sem,
          u_sem, gp_sem, pf_sem, dz_sem, f_send, b_send,
          y_loc, y_send, x_loc, x_send, yr_send, xr_send, wu_sem, wd_sem, wo_sem):
    s = lax.axis_index('stage')
    first = s == 0
    last = s == n_st - 1
    w = _pick(s, WARM)
    par_y = _pick(s, PAR_Y)
    off_p = _pick(s, OFF_P)
    off_s = _pick(s, OFF_S)
    lag_x = _pick(s, LAG_X)
    f_dim = w1.shape[1]
    d_dim = w1.shape[0]

    def local(src, dst, sem):
        return pltpu.make_async_copy(src, dst, sem)

    def remote(src, dst, ssem, rsem, dev):
        return pltpu.make_async_remote_copy(
            src_ref=src, dst_ref=dst, send_sem=ssem, recv_sem=rsem,
            device_id={'stage': dev}, device_id_type=pl.DeviceIdType.MESH)

    @pl.when(first)
    def _():
        local(x.at[0], h_all.at[0], h_recv.at[0]).start()
    local(w1h, w1, w_sem.at[0]).start()
    local(w2h, w2, w_sem.at[1]).start()
    barrier = pltpu.get_barrier_semaphore()
    for k in range(1, n_st):
        pl.semaphore_signal(barrier, inc=1, device_id={'stage': lax.rem(s + k, n_st)},
                            device_id_type=pl.DeviceIdType.MESH)
    pl.semaphore_wait(barrier, n_st - 1)

    @pl.when(last)
    def _():
        def go(m, c):
            local(gin.at[m], g_all.at[m], g_recv.at[m]).start()
            return c
        lax.fori_loop(0, n, go, 0)
    local(w1h, w1, w_sem.at[0]).wait()
    local(w2h, w2, w_sem.at[1]).wait()

    @pl.when(first)
    def _():
        def go(m, c):
            local(x.at[m], h_all.at[m], h_recv.at[m]).start()
            return c
        lax.fori_loop(1, n, go, 0)

    relay_y = (s == 1) | (s == 3) | (s == 5)
    relay_x = (s == 2) | (s == 4) | (s == 6)

    def second_y(m):
        return (s == 1) | ((s == 5) & (m % 2 == 0)) | ((s == 3) & (m % 2 == 1))

    def next_y(m):
        return jnp.where(s == 1, 3 + 2 * (m % 2), 1)

    def pass_y(m):
        local(y.at[m], y.at[m], y_recv.at[m]).wait()

        @pl.when(relay_y)
        def _():
            remote(y.at[m], y.at[m], yr_send.at[0, m], y_recv.at[m], s - 1).start()

        @pl.when(second_y(m))
        def _():
            remote(y.at[m], y.at[m], yr_send.at[1, m], y_recv.at[m], next_y(m)).start()

    def pass_x(m):
        local(dx.at[m], dx.at[m], x_recv.at[m]).wait()

        @pl.when(relay_x)
        def _():
            remote(dx.at[m], dx.at[m], xr_send.at[0, m], x_recv.at[m], s + 1).start()

        @pl.when(s == 2)
        def _():
            remote(dx.at[m], dx.at[m], xr_send.at[1, m], x_recv.at[m], 6).start()

    def wait_f_send(sl):
        remote(of.at[sl], h_all.at[0], f_send.at[sl], h_recv.at[0], s + 1).wait_send()

    def wait_b_send(sl):
        @pl.when(first)
        def _():
            local(ob.at[sl], dx.at[0], x_loc.at[sl]).wait()
            for k, dev in enumerate((1, 2, 4)):
                remote(ob.at[sl], dx.at[0], x_send.at[k, sl], x_recv.at[0], dev).wait_send()

        @pl.when(jnp.logical_not(first))
        def _():
            remote(ob.at[sl], g_all.at[0], b_send.at[sl], g_recv.at[0], s - 1).wait_send()

    def wait_f_store(sl):
        local(u.at[sl], us.at[0], u_sem.at[sl]).wait()
        local(gp.at[sl], gps.at[0], gp_sem.at[sl]).wait()

    def forward(m):
        sl = m % NF
        su = m % 2
        local(h_all.at[m], h_all.at[m], h_recv.at[m]).wait()
        local(h_all.at[m], hs.at[m], hs_sem).start()

        @pl.when(jnp.logical_not(last) & (m >= NF))
        def _():
            wait_f_send(sl)
        h = h_all.at[m]
        with jax.named_scope('F'):
            for j in range(f_dim // FT):
                c = pl.ds(j * FT, FT)
                z = jnp.dot(h[...], w1[:, c], preferred_element_type=F32)
                uu, gg = _gelu(z)
                u[su, :, c] = uu.astype(BF)
                gp[su, :, c] = gg
            for j in range(d_dim // OT):
                c = pl.ds(j * OT, OT)
                r = jnp.dot(u[su], w2[:, c], preferred_element_type=F32)
                of[sl, :, c] = (h[:, c].astype(F32) + r).astype(BF)

        @pl.when(last)
        def _():
            local(of.at[sl], y.at[m], y_loc.at[sl]).start()

        @pl.when(jnp.logical_not(last))
        def _():
            remote(of.at[sl], h_all.at[m], f_send.at[sl], h_recv.at[m], s + 1).start()
        local(u.at[su], us.at[m], u_sem.at[su]).start()
        local(gp.at[su], gps.at[m], gp_sem.at[su]).start()

    def backward(m):
        sl = m % 2
        gi = jnp.where(w == 1, sl, 2)
        local(g_all.at[m], g_all.at[m], g_recv.at[m]).wait()
        local(g_all.at[m], gs.at[m], gs_sem).start()

        @pl.when(w > 1)
        def _():
            local(gps.at[m], gp.at[2], pf_sem).wait()

        @pl.when(m >= 2)
        def _():
            wait_b_send(sl)

        @pl.when(m >= 1)
        def _():
            local(dz, dzs.at[0], dz_sem).wait()
        g = g_all.at[m]
        with jax.named_scope('B'):
            for j in range(f_dim // FT):
                c = pl.ds(j * FT, FT)
                du = lax.dot_general(g[...], w2[c, :], NT, preferred_element_type=F32)
                dz[:, c] = (gp[gi, :, c] * du).astype(BF)
            local(dz, dzs.at[m], dz_sem).start()
            for j in range(d_dim // OT):
                c = pl.ds(j * OT, OT)
                r = lax.dot_general(dz[...], w1[c, :], NT, preferred_element_type=F32)
                ob[sl, :, c] = (g[:, c].astype(F32) + r).astype(BF)

        @pl.when(first)
        def _():
            for k, dev in enumerate((1, 2, 4)):
                remote(ob.at[sl], dx.at[m], x_send.at[k, sl], x_recv.at[m], dev).start()
            local(ob.at[sl], dx.at[m], x_loc.at[sl]).start()

        @pl.when(jnp.logical_not(first))
        def _():
            remote(ob.at[sl], g_all.at[m], b_send.at[sl], g_recv.at[m], s - 1).start()

    n_grp = f_dim // FT

    def w_load(i):
        c = pl.ds(pl.multiple_of(i * FT, FT), FT)
        sl = i % 2
        for k in range(KB):
            to = pl.ds(k * FT, FT)
            local(us.at[k, :, c], u.at[2 * sl, :, to], wu_sem.at[sl]).start()
            local(dzs.at[k, :, c], u.at[2 * sl + 1, :, to], wd_sem.at[sl]).start()

    def w_group(i):
        sl = i % 2

        @pl.when(i + 1 < n_grp)
        def _():
            w_load(i + 1)
        local(us.at[0], u.at[2 * sl], wu_sem.at[sl]).wait()
        local(dzs.at[0], u.at[2 * sl + 1], wd_sem.at[sl]).wait()

        @pl.when(i >= 2)
        def _():
            local(gp.at[sl], gps.at[0], wo_sem.at[sl]).wait()
        kt = KB * h_all.shape[1]
        b = h_all.shape[1]
        with jax.named_scope('W'):
            lhs = jnp.concatenate([u[2 * sl, :, k * FT:(k + 1) * FT] for k in range(KB)], axis=0)
            r = lax.dot_general(lhs, g_all[0:KB].reshape(kt, d_dim), TN, preferred_element_type=F32)
            for q in range(FT // b):
                gp[sl, :, d_dim * q:d_dim * (q + 1)] = r[b * q:b * (q + 1)]
            rhs = jnp.concatenate([u[2 * sl + 1, :, k * FT:(k + 1) * FT] for k in range(KB)], axis=0)
            r = lax.dot_general(h_all[0:KB].reshape(kt, d_dim), rhs, TN, preferred_element_type=F32)
            for q in range(d_dim // b):
                gp[sl, :, 2 * d_dim + FT * q:2 * d_dim + FT * (q + 1)] = r[b * q:b * (q + 1)]
        for q in range(FT // b):
            local(gp.at[sl, :, pl.ds(d_dim * q, d_dim)],
                  p2.at[pl.ds(pl.multiple_of(i * FT + b * q, b), b), :], wo_sem.at[sl]).start()
        for q in range(d_dim // b):
            local(gp.at[sl, :, pl.ds(2 * d_dim + FT * q, FT)],
                  p1.at[pl.ds(b * q, b), pl.ds(pl.multiple_of(i * FT, FT), FT)], wo_sem.at[sl]).start()

    t0 = _pick(s, T_W)
    gap = jnp.where(s <= 1, 3, 0)
    ticks = jnp.maximum(jnp.maximum(n + w, t0 + n_grp + gap), n + 2)

    def send_y(m):
        remote(y.at[m], y.at[m], y_send.at[0, m], y_recv.at[m], 6).start()
        remote(y.at[m], y.at[m], y_send.at[1, m], y_recv.at[m], 5 - 2 * (m % 2)).start()

    def tick(t, c):
        @pl.when((t >= 2) & (t < n + 2))
        def _():
            wait_f_store(t % 2)

        @pl.when(last & (t >= 2) & (t < n + 2))
        def _():
            local(of.at[(t - 2) % NF], y.at[0], y_loc.at[(t - 2) % NF]).wait()

            @pl.when(t - 2 < YC)
            def _():
                send_y(t - 2)
        for at, m in LATE_Y.items():
            @pl.when(last & (t == at))
            def _(m=m):
                send_y(m)

        @pl.when((t >= w) & (t - w < n))
        def _():
            backward(t - w)

        @pl.when((w > 1) & (t - w + 1 >= 0) & (t - w + 1 < n))
        def _():
            local(gps.at[t - w + 1], gp.at[2], pf_sem).start()

        @pl.when(t < n)
        def _():
            forward(t)

        k = t - t0
        grp = jnp.where(k < 4, k, k - gap)

        @pl.when((k >= 0) & ((k < 4) | (k - gap >= 4)) & (grp < n_grp))
        def _():
            w_group(grp)

        @pl.when(t == t0 - 1)
        def _():
            w_load(0)

        mp = t - off_p

        @pl.when((mp >= 0) & (mp < YC) & (mp % 2 == par_y))
        def _():
            pass_y(mp)
        ml = t - (n + w + 2) + YC

        @pl.when(relay_y & (ml >= YC) & (ml < n) & (ml % 2 == par_y))
        def _():
            pass_y(ml)
        ms = t - off_s

        @pl.when((ms >= 0) & (ms < YC) & (ms % 2 != par_y))
        def _():
            pass_y(ms)
        mx = t - w - lag_x

        @pl.when(relay_x & (mx >= 0) & (mx < n))
        def _():
            pass_x(mx)
        return c
    lax.fori_loop(0, ticks, tick, 0)

    x0 = jnp.where(relay_x, jnp.clip(ticks - w - lag_x, 0, n), jnp.where(first, n, 0))

    def left_p(m):
        at = jnp.where(m < YC, m + off_p, jnp.where(relay_y, n + w + 2 + m - YC, 999))
        return (m % 2 == par_y) & (at >= ticks)

    def left_s(m):
        at = jnp.where(m < YC, m + off_s, 999)
        return (m % 2 != par_y) & (at >= ticks)

    def rest_p(m, c):
        @pl.when(left_p(m) | ((s == 1) & left_s(m)))
        def _():
            pass_y(m)
        return c

    def rest_s(m, c):
        @pl.when(left_s(m) & (s != 1))
        def _():
            pass_y(m)
        return c

    def rest_x(m, c):
        pass_x(m)
        return c
    early = jnp.where(relay_y, 0, n)
    late = jnp.where(relay_y | last, n, 0)
    lax.fori_loop(early, n, rest_p, 0)
    lax.fori_loop(early, n, rest_s, 0)
    lax.fori_loop(x0, n, rest_x, 0)
    lax.fori_loop(late, n, rest_p, 0)
    lax.fori_loop(late, n, rest_s, 0)

    @pl.when(jnp.logical_not(last))
    def _():
        for m in range(n - NF, n):
            wait_f_send(m % NF)
    for m in (n - 2, n - 1):
        wait_b_send(m % 2)
        local(gp.at[m % 2], gps.at[0], wo_sem.at[m % 2]).wait()
    local(dz, dzs.at[0], dz_sem).wait()
    local(h_all, hs, hs_sem).wait()
    local(g_all, gs, gs_sem).wait()

    def done(m, c):
        @pl.when(last)
        def _():
            for k in range(2):
                remote(y.at[m], y.at[m], y_send.at[k, m], y_recv.at[m], 6).wait_send()

        @pl.when(relay_y)
        def _():
            remote(y.at[m], y.at[m], yr_send.at[0, m], y_recv.at[m], s - 1).wait_send()

        @pl.when(second_y(m))
        def _():
            remote(y.at[m], y.at[m], yr_send.at[1, m], y_recv.at[m], next_y(m)).wait_send()

        @pl.when(relay_x)
        def _():
            remote(dx.at[m], dx.at[m], xr_send.at[0, m], x_recv.at[m], s + 1).wait_send()

        @pl.when(s == 2)
        def _():
            remote(dx.at[m], dx.at[m], xr_send.at[1, m], x_recv.at[m], 6).wait_send()
        return c
    lax.fori_loop(0, n, done, 0)


def _run_pipe(n_st, x, g, w1, w2):
    n, b, d = x.shape
    f = w1.shape[1]
    act = jax.ShapeDtypeStruct((n, b, d), BF)
    wide = jax.ShapeDtypeStruct((n, b, f), BF)
    anyspec = pl.BlockSpec(memory_space=pl.ANY)
    dma = pltpu.SemaphoreType.DMA
    return pl.pallas_call(
        functools.partial(_pipe, n, n_st),
        out_shape=(act, act, act, act, wide, wide, jax.ShapeDtypeStruct((n, b, f), F32),
                   jax.ShapeDtypeStruct((d, f), F32), jax.ShapeDtypeStruct((f, d), F32)),
        in_specs=[anyspec] * 4,
        out_specs=(anyspec,) * 9,
        scratch_shapes=[
            pltpu.VMEM((d, f), BF), pltpu.VMEM((f, d), BF),
            pltpu.VMEM((n, b, d), BF), pltpu.VMEM((n, b, d), BF),
            pltpu.VMEM((4, b, f), BF), pltpu.VMEM((3, b, f), F32), pltpu.VMEM((b, f), BF),
            pltpu.VMEM((NF, b, d), BF), pltpu.VMEM((2, b, d), BF),
            dma((2,)), dma((n,)), dma((n,)), dma((n,)), dma((n,)), dma, dma,
            dma((2,)), dma((2,)), dma, dma, dma((NF,)), dma((2,)),
            dma((NF,)), dma((2, n)), dma((2,)), dma((3, 2)), dma((2, n)), dma((2, n)),
            dma((2,)), dma((2,)), dma((2,)),
        ],
        compiler_params=pltpu.CompilerParams(has_side_effects=True, collective_id=0, vmem_limit_bytes=67043328),
    )(x, g, w1, w2)


def _finish(u, dz, h, g, p1, p2, y, dx, o1, o2, yo, dxo):
    o2[...] = p2[...] + lax.dot_general(u[...], g[...], TN, preferred_element_type=F32)
    o1[...] = p1[...] + lax.dot_general(h[...], dz[...], TN, preferred_element_type=F32)
    yo[...] = y[...]
    dxo[...] = dx[...]


def _run_finish(us, dzs, hs, gs, p1, p2, y, dx):
    n, b, d = y.shape
    f = us.shape[1]
    k = (n - KB) * b
    steps = f // FT
    m = n // steps
    one = pl.Buffered(1)
    act = pl.BlockSpec((m, b, d), lambda j: (j, 0, 0))
    col = pl.BlockSpec((d, FT), lambda j: (0, j))
    row = pl.BlockSpec((FT, d), lambda j: (j, 0))
    tok = pl.BlockSpec((k, FT), lambda j: (1, j))
    all_d = pl.BlockSpec((k, d), lambda j: (1, 0), pipeline_mode=one)
    return pl.pallas_call(
        _finish,
        grid=(steps,),
        out_shape=(jax.ShapeDtypeStruct((d, f), F32), jax.ShapeDtypeStruct((f, d), F32),
                   jax.ShapeDtypeStruct((n, b, d), BF), jax.ShapeDtypeStruct((n, b, d), BF)),
        in_specs=[tok, tok, all_d, all_d, col, row, act, act],
        out_specs=[col, row, act, act],
        compiler_params=pltpu.CompilerParams(vmem_limit_bytes=63 * 1024 * 1024),
    )(us, dzs, hs, gs, p1, p2, y, dx)


def solution(mesh):
    n_st = mesh.shape['stage']

    def body(x, g, w1, w2):
        n, b, d = x.shape
        f = w1.shape[2]
        y, dx, hs, gs, us, dzs, _, p1, p2 = _run_pipe(n_st, x, g, w1[0], w2[0])
        dw1, dw2, y, dx = _run_finish(us.reshape(n * b, f), dzs.reshape(n * b, f), hs.reshape(n * b, d),
                                      gs.reshape(n * b, d), p1, p2, y, dx)
        return y, dx, dw1[None], dw2[None]

    return jax.shard_map(body, mesh=mesh,
                         in_specs=(P('data'), P('data'), P('stage'), P('stage')),
                         out_specs=(P('data'), P('data'), P(('data', 'stage')), P(('data', 'stage'))),
                         check_vma=False)
```
